32 devices in a mesh: row: 4 (over y, core), col: 8 (over z, x).
Axes of the slice: x: 2, y: 2, z: 4, core: 2. Of those that a mesh axis runs over, the one named last changes fastest.
Arguments:
- fluid_data: float32 [51, 8192], P(None, ('row', 'col')), as said below
- center_data: float32 [51, 8192], P(None, ('col', 'row')), as said below
- poly_coef: float32 [48, 4], replicated, may hold values from -3 to 3
Outputs:
- fluid_motion: float32 [48, 8192], P(None, ('row', 'col'))
- center_load: float32 [48, 8192], P(None, ('col', 'row'))
The draws below stay inside these ranges and needn't reach their ends.
Inputs may be any that keep to these rules, and one draw needn't show every extreme that they name: Rows 0 to 2 of fluid_data lie in [0, 1]; rows 3 and on are forces. Rows 0 and 1 of center_data lie in [0, 1] and row 2 lies in [-0.5, -0.02], so every center is at least 0.02 below every vertex; rows 3 and on are coefficients.
All inputs are finite; a program needn't handle non-finite values.
Results may differ from the reference program's by a relative error of at most 0.0003.
Values sent between devices are 32-bit elements; how exact they have to be, the bound alone decides.
A program may use at most 64 MiB of HBM per device.

```python
import math
import jax
import jax.numpy as jnp
from jax import lax

WAVES = 64
COLS = 48
FLUID = 8192
CENTERS = 8192


def draw_fluid_data(key, part):
    first, second = jax.random.split(jax.random.fold_in(key, 11))
    places = jax.random.uniform(first, (3, FLUID), jnp.float32)
    spread = 2.0 * math.pi * WAVES * math.sqrt(0.8 / FLUID)
    values = jax.random.normal(second, (COLS, FLUID), jnp.float32) * spread
    return jnp.concatenate([places, values], axis=0)


def draw_center_data(key, part):
    first, second, third = jax.random.split(jax.random.fold_in(key, 23), 3)
    plane = jax.random.uniform(first, (2, CENTERS), jnp.float32)
    depth = jax.random.uniform(second, (1, CENTERS), jnp.float32)
    spread = 2.0 * math.pi * WAVES * math.sqrt(0.8 / CENTERS)
    height = -0.02 - 0.48 * depth
    values = jax.random.normal(third, (COLS, CENTERS), jnp.float32) * spread
    return jnp.concatenate([plane, height, values], axis=0)


def noise(key, dims, scale, limit, kind=jnp.bfloat16):
    entries = scale * jax.random.normal(key, dims, jnp.float32)
    return jnp.clip(entries, min=-limit, max=limit).astype(kind)


def setup_inputs(seed: int = 0) -> dict:
    streams_of = jax.random.split(jax.random.key(seed), 4)
    fluid_data = draw_fluid_data(jax.random.fold_in(streams_of[3], 71), 0)
    center_data = draw_center_data(jax.random.fold_in(streams_of[3], 71), 0)
    poly_coef = noise(streams_of[2], (COLS, 4), 0.5, 3.0, jnp.float32)
    return dict(fluid_data=fluid_data, center_data=center_data, poly_coef=poly_coef)


def kernel_block(center_pos, fluid_pos):
    dx = center_pos[0][:, None] - fluid_pos[0][None, :]
    dy = center_pos[1][:, None] - fluid_pos[1][None, :]
    dz = center_pos[2][:, None] - fluid_pos[2][None, :]
    sq = dx * dx + dy * dy + dz * dz
    phase = 2.0 * math.pi * WAVES * jnp.sqrt(sq)
    return jnp.sin(phase) / phase

def reference(fluid_data, center_data, poly_coef):
    total = center_data.shape[1]
    width = fluid_data.shape[1]
    block = math.gcd(total, 256)
    count = total // block
    fluid_pos = fluid_data[:3]
    forces = fluid_data[3:]
    pieces = center_data.reshape(center_data.shape[0], count, block).transpose(1, 0, 2)

    def step(motion, piece):
        tile = kernel_block(piece[:3], fluid_pos)
        motion = motion + jnp.dot(piece[3:], tile, precision=lax.Precision.HIGHEST, preferred_element_type=jnp.float32)
        back = lax.dot_general(forces, tile, (((1,), (1,)), ((), ())), precision=lax.Precision.HIGHEST, preferred_element_type=jnp.float32)
        return (motion, back)
    start = jnp.zeros((forces.shape[0], width), jnp.float32)
    motion, backs = lax.scan(step, start, pieces)
    loads = backs.transpose(1, 0, 2).reshape(forces.shape[0], total)
    affine = poly_coef[:, 0:1] + jnp.dot(poly_coef[:, 1:], fluid_pos, precision=lax.Precision.HIGHEST, preferred_element_type=jnp.float32)
    return (motion + affine, loads)
```

```python
import functools

import jax
import jax.numpy as jnp
from jax import lax
from jax.experimental import pallas as pl
from jax.experimental.pallas import tpu as pltpu
from jax.sharding import PartitionSpec as P

WAVES = 64
MESH = pl.DeviceIdType.MESH
TOP = 12.404427306735432
MID = 0.6418441597071612
LOW = 0.16126480593510223
DEPTH = 128


def paired(me, m, n):
    other, bit = 0, 1
    while bit < n:
        other = other + (((me // bit) % 2 + (m // bit) % 2) % 2) * bit
        bit *= 2
    return other


def dot(a, b, dims):
    return lax.dot_general(a, b, (dims, ((), ())), preferred_element_type=jnp.float32)


def rounded(x):
    return x.astype(jnp.bfloat16).astype(jnp.float32)


def split(x):
    high = x.astype(jnp.bfloat16)
    low = (x - high.astype(jnp.float32)).astype(jnp.bfloat16)
    return high, low


def pieces(places):
    x = places * float(WAVES)
    coarse = jnp.round(x * 2.0) * 0.5
    fine = x - coarse
    coarse = coarse - float(WAVES // 2)
    first = rounded(fine)
    second = rounded(fine - first)
    fine = first + second
    large = coarse * coarse
    small = fine * (coarse + coarse) + fine * fine
    large = large[0:1] + large[1:2] + large[2:3]
    small = small[0:1] + small[1:2] + small[2:3]
    l1 = rounded(large)
    l2 = large - l1
    s1 = rounded(small)
    s2 = rounded(small - s1)
    s3 = small - s1 - s2
    return coarse, first, second, (l1, l2), (s1, s2, s3)


def rows_of(base, at, extra):
    out = jnp.where(at < 3, base, 0.0)
    for i, e in extra:
        out = jnp.where(at == i, e, out)
    return out


def center_rows(places):
    c, f1, f2, large, small = pieces(places)
    at = lax.broadcasted_iota(jnp.int32, places.shape, 0)
    one = 1.0
    return [
        rows_of(c, at, [(3, large[0]), (4, large[1]), (5, one), (6, one)]),
        rows_of(c, at, [(3, small[0]), (4, small[1]), (5, small[2])]),
        rows_of(c, at, [(3, one), (4, one), (5, one)]),
        rows_of(f1, at, []),
        rows_of(f2, at, []),
        rows_of(f1, at, []),
        rows_of(f1, at, []),
        rows_of(f2, at, []),
        rows_of(f2, at, []),
    ]


def fluid_rows(places):
    c, f1, f2, large, small = pieces(places)
    at = lax.broadcasted_iota(jnp.int32, places.shape, 0)
    one = 1.0
    c, f1, f2 = -2.0 * c, -2.0 * f1, -2.0 * f2
    return [
        rows_of(c, at, [(3, one), (4, one), (5, large[0]), (6, large[1])]),
        rows_of(f1, at, [(3, one), (4, one), (5, one)]),
        rows_of(f2, at, [(3, small[0]), (4, small[1]), (5, small[2])]),
        rows_of(c, at, []),
        rows_of(c, at, []),
        rows_of(f1, at, []),
        rows_of(f2, at, []),
        rows_of(f1, at, []),
        rows_of(f2, at, []),
    ]


def tiles_of(S, T):
    half = T // 2
    near = list(range(1, min(half, 3)))
    order = [(0, 0), (0, half)]
    order += [(0, p) for p in near] + [(1, p) for p in near]
    for p in near:
        order += [(0, half + p), (1, half + p)]
    for p in range(3, half):
        order += [(0, p), (1, p), (0, half + p), (1, half + p)]
    for m in range(S - 1, 2, -1):
        order += [(m, r) for r in [0, half] + list(range(1, half)) + list(range(half + 1, T))]
    order += [(2, r) for r in list(range(T - 1, half, -1)) + list(range(half - 1, 0, -1)) + [half, 0]]
    order += [(1, 0), (1, half)]
    assert len(set(order)) == S * T == len(order)
    return order


def body(rows, cols, side, fluid, center, poly, motion, loads, *scratch):
    (fl, ce, pv, fa, ff, fc, chl, fhl, sq, kh, kl, mo_out, mo_in, ld_out, ld_in, pre) = scratch[:16]
    own, fs, fr, cs, cr, ms, mr, ls, lr, ps, pr = scratch[16:]
    S, T = cols // side, rows * side
    half = T // 2
    row, col = lax.axis_index("row"), lax.axis_index("col")
    my_s, my_t = col // side, (row % 2) * half + (col % side) * (rows // 2) + row // 2
    nvals = pv.shape[1]
    wf, wc = fluid.shape[1], center.shape[1]

    def along_s(m):
        return {"row": row, "col": paired(my_s, m, S) * side + col % side}

    def along_t(m):
        i = paired(my_t, m, T)
        return {
            "row": (i % (rows // 2)) * 2 + i // half,
            "col": (col // side) * side + (i % half) // (rows // 2),
        }

    def copy(src, dst, send, recv, where):
        return pltpu.make_async_remote_copy(
            src_ref=src, dst_ref=dst, send_sem=send, recv_sem=recv, device_id=where, device_id_type=MESH
        )

    def send_fluid(m):
        return copy(fl.at[0], fl.at[m], fs.at[m], fr.at[m], along_s(m))

    def send_center(p):
        return copy(ce.at[0], ce.at[p], cs.at[p], cr.at[p], along_t(p))

    def hand_on(p):
        q = p + half
        return copy(ce.at[p], ce.at[q], cs.at[q], cr.at[q], along_t(half))

    def send_motion(m):
        return copy(mo_out.at[m], mo_in.at[m], ms.at[m], mr.at[m], along_s(m))

    def send_pre(p):
        j = p - half
        return copy(ld_out.at[p], pre.at[j], ps.at[j], pr.at[j], along_t(half))

    def send_loads(j):
        return copy(ld_out.at[j], ld_in.at[j], ls.at[j], lr.at[j], along_t(j))

    def send_other():
        return copy(ld_out.at[half], ld_in.at[0], ls.at[0], lr.at[0], along_t(half))

    local = [
        pltpu.make_async_copy(center, ce.at[0], own.at[0]),
        pltpu.make_async_copy(fluid, fl.at[0], own.at[1]),
        pltpu.make_async_copy(poly, pv, own.at[2]),
    ]
    for c in local:
        c.start()
    barrier = pltpu.get_barrier_semaphore()
    for p in range(1, half + 1):
        pl.semaphore_signal(barrier, inc=1, device_id=along_t(p), device_id_type=MESH)
    for m in range(1, S):
        pl.semaphore_signal(barrier, inc=1, device_id=along_s(m), device_id_type=MESH)
    fc[...] = jnp.zeros(fc.shape, jnp.bfloat16)
    fa[...] = jnp.zeros(fa.shape, jnp.float32)
    for c in local:
        c.wait()
    pl.semaphore_wait(barrier, S - 1 + half)
    for p in [half] + list(range(1, half)):
        send_center(p).start()
    for m in [1] + list(range(S - 1, 1, -1)):
        send_fluid(m).start()

    def ready_center(r):
        for g, x in enumerate(center_rows(ce[r, 0:8, :])):
            fa[0, 8 * g : 8 * g + 8, 0:wc] = x
        depth = 8 * 9
        fc[r, 0 : depth + 8, :] = fa[0, 0 : depth + 8, 0:wc].astype(jnp.bfloat16)
        high, low = split(ce[r, 3:, :] * TOP)
        chl[r, 0:nvals] = high
        chl[r, nvals:] = low

    def ready_fluid(m):
        for g, x in enumerate(fluid_rows(fl[m, 0:8, :])):
            fa[1, 8 * g : 8 * g + 8, 0:wf] = x
        ff[m] = jnp.transpose(fa[1, :, 0:wf]).astype(jnp.bfloat16)
        high, low = split(fl[m, 3:, :] * TOP)
        fhl[m, 0:nvals] = high
        fhl[m, nvals:] = low

    def squares(tile, slot):
        m, r = tile
        sq[slot] = dot(ff[m], fc[r], ((1,), (0,)))

    def values(slot):
        step = 32 if wf % 32 == 0 else wf
        for j in range(0, wf, step):
            at = pl.ds(j, step)
            s = sq[slot, at, :]
            inv = lax.rsqrt(s)
            turns = s * inv
            f = turns - jnp.round(turns)
            size = jnp.abs(f)
            rest = 0.5 - size
            q = size * rest
            value = (f * rest * inv) * ((q + MID) * q + LOW)
            high, low = split(value)
            kh[slot, at, :] = high
            kl[slot, at, :] = low

    seen = set()

    def add(ref, i, name, x):
        if (name, i) in seen:
            ref[i] += x
        else:
            ref[i] = x
            seen.add((name, i))

    def sums(tile, slot):
        m, r = tile
        k_high, k_low = kh[slot], kl[slot]
        across = ((1,), (0,))
        wide = dot(fhl[m], k_high, across)
        add(ld_out, r, "l", wide[:nvals] + wide[nvals:] + dot(fhl[m, 0:nvals], k_low, across))
        back = ((1,), (1,))
        wide = dot(chl[r], k_high, back)
        add(mo_out, m, "m", wide[:nvals] + wide[nvals:] + dot(chl[r, 0:nvals], k_low, back))

    order = tiles_of(S, T)
    pairs = [order[i : i + 2] for i in range(0, len(order), 2)]
    have_f, have_c, handed = {0}, {0}, {0}
    left_m = {m: T for m in range(S)}
    left_r = {r: S for r in range(T)}
    waiting, sent_at = [], {}
    ready_fluid(0)
    ready_center(0)

    def receive(r):
        if r <= half and r not in handed:
            send_center(r).wait_recv()
            if r < half:
                hand_on(r).start()
            handed.add(r)

    def fetch(pair):
        fresh = []
        for m, r in pair:
            if r not in have_c:
                if r <= half:
                    receive(r)
                else:
                    receive(min(r - half + 1, half - 1))
                    hand_on(r - half).wait_recv()
                fresh.append((ready_center, r))
                have_c.add(r)
            if m not in have_f:
                send_fluid(m).wait_recv()
                fresh.append((ready_fluid, m))
                have_f.add(m)
        return fresh

    def finish(j):
        send_pre(half + j).wait_recv()
        ld_out[j] += pre[j]
        send_loads(j).start()

    def done(pair, k):
        for m, r in pair:
            left_m[m] -= 1
            left_r[r] -= 1
            if m and not left_m[m]:
                send_motion(m).start()
            if r and not left_r[r]:
                if r > half:
                    send_pre(r).start()
                    sent_at[r] = k
                elif r == half:
                    send_other().start()
                else:
                    waiting.append(r)

    slot_of = lambda k, i: (k % 2) * 2 + i
    for f, i in fetch(pairs[0]):
        f(i)
    for i in range(2):
        squares(pairs[0][i], slot_of(0, i))
    for i in range(2):
        values(slot_of(0, i))
    n = len(pairs)
    for k in range(n + 1):
        fresh = fetch(pairs[k + 1]) if k + 1 < n else []
        for i in range(2):
            if k > 1:
                sums(pairs[k - 1][i], slot_of(k - 1, i))
            if k == 0:
                sums(pairs[0][i], slot_of(0, i))
        for f, i in fresh:
            f(i)
        for i in range(2):
            if k + 1 < n:
                squares(pairs[k + 1][i], slot_of(k + 1, i))
        for i in range(2):
            if 0 < k < n:
                values(slot_of(k, i))
        if k > 0:
            done(pairs[k - 1], k)
            for j in list(waiting):
                if k >= sent_at.get(half + j, n) + 3 or k == n:
                    finish(j)
                    waiting.remove(j)

    total = mo_out[0]
    affine = jnp.transpose(pv[...])
    for a in range(3):
        total = total + affine[:, a + 1 : a + 2] * fl[0, a : a + 1, :]
    total = total + affine[:, 0:1]
    order_s = list(range(S - 1, 0, -1))
    for m in order_s:
        send_motion(m).wait_recv()
        total = total + mo_in[m]
    motion[...] = total
    total = ld_out[0]
    send_other().wait_recv()
    total = total + ld_in[0]
    for j in range(half - 1, 0, -1):
        send_loads(j).wait_recv()
        total = total + ld_in[j]
    loads[...] = total
    for m in order_s:
        send_fluid(m).wait_send()
        send_motion(m).wait_send()
    for p in range(1, half + 1):
        send_center(p).wait_send()
    for p in range(1, half):
        hand_on(p).wait_send()
        send_pre(p + half).wait_send()
        send_loads(p).wait_send()
    send_other().wait_send()


def per_device(rows, cols, side, fluid_data, center_data, poly_coef):
    f32, bf16 = jnp.float32, jnp.bfloat16
    S, T = cols // side, rows * side
    height, wf = fluid_data.shape
    wc = center_data.shape[1]
    n = height - 3
    vmem = pl.BlockSpec(memory_space=pltpu.VMEM)
    hbm = pl.BlockSpec(memory_space=pltpu.HBM)
    sems = [pltpu.SemaphoreType.DMA((k,)) for k in (3, S, S, T, T, S, S, T // 2, T // 2, T // 2, T // 2)]
    return pl.pallas_call(
        functools.partial(body, rows, cols, side),
        out_shape=(jax.ShapeDtypeStruct((n, wf), f32), jax.ShapeDtypeStruct((n, wc), f32)),
        in_specs=[hbm] * 3,
        out_specs=(vmem, vmem),
        scratch_shapes=[
            pltpu.VMEM((S, height, wf), f32),
            pltpu.VMEM((T, height, wc), f32),
            pltpu.VMEM((4, n), f32),
            pltpu.VMEM((2, DEPTH, max(wf, wc)), f32),
            pltpu.VMEM((S, wf, DEPTH), bf16),
            pltpu.VMEM((T, DEPTH, wc), bf16),
            pltpu.VMEM((T, 2 * n, wc), bf16),
            pltpu.VMEM((S, 2 * n, wf), bf16),
            pltpu.VMEM((4, wf, wc), f32),
            pltpu.VMEM((4, wf, wc), bf16),
            pltpu.VMEM((4, wf, wc), bf16),
            pltpu.VMEM((S, n, wf), f32),
            pltpu.VMEM((S, n, wf), f32),
            pltpu.VMEM((T, n, wc), f32),
            pltpu.VMEM((T // 2, n, wc), f32),
            pltpu.VMEM((T // 2, n, wc), f32),
            *sems,
        ],
        compiler_params=pltpu.CompilerParams(
            collective_id=0, has_side_effects=True, vmem_limit_bytes=67_043_328
        ),
    )(fluid_data, center_data, poly_coef.T)


def solution(mesh):
    rows, cols = mesh.shape["row"], mesh.shape["col"]
    side = 2 if cols % 2 == 0 else 1
    placed = (P(None, ("row", "col")), P(None, ("col", "row")), P())
    return jax.shard_map(
        functools.partial(per_device, rows, cols, side),
        mesh=mesh,
        in_specs=placed,
        out_specs=(P(None, ("row", "col")), P(None, ("col", "row"))),
        check_vma=False,
    )
```

```python
import functools

import jax
import jax.numpy as jnp
from jax import lax
from jax.experimental import pallas as pl
from jax.experimental.pallas import tpu as pltpu
from jax.sharding import PartitionSpec as P

WAVES = 64
MESH = pl.DeviceIdType.MESH
TOP = 12.404427306735432
MID = 0.6418441597071612
LOW = 0.16126480593510223
DEPTH = 128


def paired(me, m, n):
    other, bit = 0, 1
    while bit < n:
        other = other + (((me // bit) % 2 + (m // bit) % 2) % 2) * bit
        bit *= 2
    return other


def dot(a, b, dims):
    return lax.dot_general(a, b, (dims, ((), ())), preferred_element_type=jnp.float32)


def rounded(x):
    return x.astype(jnp.bfloat16).astype(jnp.float32)


def split(x):
    high = x.astype(jnp.bfloat16)
    low = (x - high.astype(jnp.float32)).astype(jnp.bfloat16)
    return high, low


def pieces(places):
    x = places * float(WAVES)
    coarse = jnp.round(x * 2.0) * 0.5
    fine = x - coarse
    coarse = coarse - float(WAVES // 2)
    first = rounded(fine)
    second = rounded(fine - first)
    fine = first + second
    large = coarse * coarse
    small = fine * (coarse + coarse) + fine * fine
    large = large[0:1] + large[1:2] + large[2:3]
    small = small[0:1] + small[1:2] + small[2:3]
    l1 = rounded(large)
    l2 = large - l1
    s1 = rounded(small)
    s2 = rounded(small - s1)
    s3 = small - s1 - s2
    return coarse, first, second, (l1, l2), (s1, s2, s3)


def rows_of(base, at, extra):
    out = jnp.where(at < 3, base, 0.0)
    for i, e in extra:
        out = jnp.where(at == i, e, out)
    return out


def center_rows(places):
    c, f1, f2, large, small = pieces(places)
    at = lax.broadcasted_iota(jnp.int32, places.shape, 0)
    one = 1.0
    return [
        rows_of(c, at, [(3, large[0]), (4, large[1]), (5, one), (6, one)]),
        rows_of(c, at, [(3, small[0]), (4, small[1]), (5, small[2])]),
        rows_of(c, at, [(3, one), (4, one), (5, one)]),
        rows_of(f1, at, []),
        rows_of(f2, at, []),
        rows_of(f1, at, []),
        rows_of(f1, at, []),
        rows_of(f2, at, []),
        rows_of(f2, at, []),
    ]


def fluid_rows(places):
    c, f1, f2, large, small = pieces(places)
    at = lax.broadcasted_iota(jnp.int32, places.shape, 0)
    one = 1.0
    c, f1, f2 = -2.0 * c, -2.0 * f1, -2.0 * f2
    return [
        rows_of(c, at, [(3, one), (4, one), (5, large[0]), (6, large[1])]),
        rows_of(f1, at, [(3, one), (4, one), (5, one)]),
        rows_of(f2, at, [(3, small[0]), (4, small[1]), (5, small[2])]),
        rows_of(c, at, []),
        rows_of(c, at, []),
        rows_of(f1, at, []),
        rows_of(f2, at, []),
        rows_of(f1, at, []),
        rows_of(f2, at, []),
    ]


def plan_of(S, T):
    half = T // 2
    near = list(range(1, min(half, 3)))
    far = list(range(3, half))
    groups = [([("c", half)], [(0, 0), (0, half)])]
    first = [(0, p) for p in near] + [(1, p) for p in near]
    groups.append(([("c", p) for p in near] + [("f", 1)], first))
    more = [("c", p) for p in far[:1]] + [("c", half + p) for p in near]
    tiles = [(m, half + p) for p in near for m in (0, 1)]
    tiles += [(m, p) for p in far[:1] for m in (0, 1)]
    groups.append((more, tiles))
    for p in far[1:]:
        groups.append(([("c", p), ("c", half + p - 1)], [(0, p), (1, p), (0, half + p - 1), (1, half + p - 1)]))
    last = far[-1:]
    every = [0, half] + list(range(1, half)) + list(range(half + 1, T))
    tiles = [(m, half + p) for p in last for m in (0, 1)] + [(2, r) for r in every]
    groups.append(([("c", half + p) for p in last] + [("f", 2)], tiles))
    for m in range(S - 2, 2, -1):
        groups.append(([("f", m)], [(m, r) for r in every]))
    tiles = [(S - 1, r) for r in list(range(T - 1, half, -1)) + list(range(half - 1, 0, -1)) + [half, 0]]
    tiles += [(1, 0), (1, half)]
    groups.append(([("f", S - 1)], tiles))
    order, needs = [], {}
    for need, tiles in groups:
        needs[len(order) // 2] = need
        order += tiles
    assert len(set(order)) == S * T == len(order)
    return [order[i : i + 2] for i in range(0, len(order), 2)], needs


def body(rows, cols, side, fluid, center, poly, out, *scratch):
    (fl, ce, pv, fa, ff, fc, chl, fhl, sq, kh, kl, mo_out, mo_in, ld_out, ld_in, pre) = scratch[:16]
    own, fs, fr, cs, cr, ms, mr, ls, lr, ps, pr = scratch[16:]
    S, T = cols // side, rows * side
    half = T // 2
    row, col = lax.axis_index("row"), lax.axis_index("col")
    my_s, my_t = col // side, (row % 2) * half + (col % side) * (rows // 2) + row // 2
    nvals = pv.shape[1]
    wf, wc = fluid.shape[1], center.shape[1]

    def along_s(m):
        return {"row": row, "col": paired(my_s, m, S) * side + col % side}

    def along_t(m):
        i = paired(my_t, m, T)
        return {
            "row": (i % (rows // 2)) * 2 + i // half,
            "col": (col // side) * side + (i % half) // (rows // 2),
        }

    def copy(src, dst, send, recv, where):
        return pltpu.make_async_remote_copy(
            src_ref=src, dst_ref=dst, send_sem=send, recv_sem=recv, device_id=where, device_id_type=MESH
        )

    def send_fluid(m):
        return copy(fl.at[0], fl.at[m], fs.at[m], fr.at[m], along_s(m))

    def send_center(p):
        return copy(ce.at[0], ce.at[p], cs.at[p], cr.at[p], along_t(p))

    def hand_on(p):
        q = p + half
        return copy(ce.at[p], ce.at[q], cs.at[q], cr.at[q], along_t(half))

    def send_motion(m):
        return copy(mo_out.at[m], mo_in.at[m], ms.at[m], mr.at[m], along_s(m))

    def send_pre(p):
        j = p - half
        return copy(ld_out.at[p], pre.at[j], ps.at[j], pr.at[j], along_t(half))

    def send_loads(j):
        return copy(ld_out.at[j], ld_in.at[j], ls.at[j], lr.at[j], along_t(j))

    def send_other():
        return copy(ld_out.at[half], ld_in.at[0], ls.at[0], lr.at[0], along_t(half))

    local = [
        pltpu.make_async_copy(center, ce.at[0], own.at[0]),
        pltpu.make_async_copy(fluid, fl.at[0], own.at[1]),
        pltpu.make_async_copy(poly, pv, own.at[2]),
    ]
    for c in local:
        c.start()
    barrier = pltpu.get_barrier_semaphore()
    for p in range(1, half + 1):
        pl.semaphore_signal(barrier, inc=1, device_id=along_t(p), device_id_type=MESH)
    for m in range(1, S):
        pl.semaphore_signal(barrier, inc=1, device_id=along_s(m), device_id_type=MESH)
    fc[...] = jnp.zeros(fc.shape, jnp.bfloat16)
    fa[...] = jnp.zeros(fa.shape, jnp.float32)
    for c in local:
        c.wait()
    pl.semaphore_wait(barrier, S - 1 + half)
    for p in [half] + list(range(1, half)):
        send_center(p).start()
    for m in [1] + list(range(2, S)):
        send_fluid(m).start()

    def ready_center(r):
        for g, x in enumerate(center_rows(ce[r, 0:8, :])):
            fa[0, 8 * g : 8 * g + 8, 0:wc] = x
        depth = 8 * 9
        fc[r, 0 : depth + 8, :] = fa[0, 0 : depth + 8, 0:wc].astype(jnp.bfloat16)
        high, low = split(ce[r, 3:, :] * TOP)
        chl[r, 0:nvals] = high
        chl[r, nvals:] = low

    def ready_fluid(m):
        for g, x in enumerate(fluid_rows(fl[m, 0:8, :])):
            fa[1, 8 * g : 8 * g + 8, 0:wf] = x
        ff[m] = jnp.transpose(fa[1, :, 0:wf]).astype(jnp.bfloat16)
        high, low = split(fl[m, 3:, :] * TOP)
        fhl[m, 0:nvals] = high
        fhl[m, nvals:] = low

    def squares(tile, slot):
        m, r = tile
        sq[slot] = dot(ff[m], fc[r], ((1,), (0,)))

    def values(slot):
        step = 32 if wf % 32 == 0 else wf
        for j in range(0, wf, step):
            at = pl.ds(j, step)
            s = sq[slot, at, :]
            inv = lax.rsqrt(s)
            turns = s * inv
            f = turns - jnp.round(turns)
            size = jnp.abs(f)
            rest = 0.5 - size
            q = size * rest
            value = (f * rest * inv) * ((q + MID) * q + LOW)
            high, low = split(value)
            kh[slot, at, :] = high
            kl[slot, at, :] = low

    seen = set()

    def add(ref, i, name, x):
        if (name, i) in seen:
            ref[i] += x
        else:
            ref[i] = x
            seen.add((name, i))

    def sums(tile, slot):
        m, r = tile
        k_high, k_low = kh[slot], kl[slot]
        across = ((1,), (0,))
        wide = dot(fhl[m], k_high, across)
        add(ld_out, r, "l", wide[:nvals] + wide[nvals:] + dot(fhl[m, 0:nvals], k_low, across))
        back = ((1,), (1,))
        wide = dot(chl[r], k_high, back)
        add(mo_out, m, "m", wide[:nvals] + wide[nvals:] + dot(chl[r, 0:nvals], k_low, back))

    pairs, needs = plan_of(S, T)
    handed = {0}
    left_m = {m: T for m in range(S)}
    left_r = {r: S for r in range(T)}
    waiting, sent_at = [], {}
    ready_fluid(0)
    ready_center(0)

    def receive(r):
        if r <= half and r not in handed:
            send_center(r).wait_recv()
            if r < half:
                hand_on(r).start()
            handed.add(r)

    def fetch(k):
        fresh = []
        for kind, i in needs.get(k, []):
            if kind == "f":
                send_fluid(i).wait_recv()
                fresh.append((ready_fluid, i))
            else:
                if i <= half:
                    receive(i)
                else:
                    hand_on(i - half).wait_recv()
                fresh.append((ready_center, i))
        return fresh

    def finish(j):
        send_pre(half + j).wait_recv()
        ld_out[j] += pre[j]
        send_loads(j).start()

    def done(pair, k):
        for m, r in pair:
            left_m[m] -= 1
            left_r[r] -= 1
            if m and not left_m[m]:
                send_motion(m).start()
            if r and not left_r[r]:
                if r > half:
                    send_pre(r).start()
                    sent_at[r] = k
                elif r == half:
                    send_other().start()
                else:
                    waiting.append(r)

    slot_of = lambda k, i: (k % 2) * 2 + i
    for f, i in fetch(0):
        f(i)
    for i in range(2):
        squares(pairs[0][i], slot_of(0, i))
    for i in range(2):
        values(slot_of(0, i))
    n = len(pairs)
    for k in range(n + 1):
        fresh = fetch(k + 1) if k + 1 < n else []
        for i in range(2):
            if k > 1:
                sums(pairs[k - 1][i], slot_of(k - 1, i))
            if k == 0:
                sums(pairs[0][i], slot_of(0, i))
        for f, i in fresh:
            f(i)
        for i in range(2):
            if k + 1 < n:
                squares(pairs[k + 1][i], slot_of(k + 1, i))
        for i in range(2):
            if 0 < k < n:
                values(slot_of(k, i))
        if k > 0:
            done(pairs[k - 1], k)
            for j in list(waiting):
                if k >= sent_at.get(half + j, n) + 2 or k == n:
                    finish(j)
                    waiting.remove(j)

    total = mo_out[0]
    affine = jnp.transpose(pv[...])
    for a in range(3):
        total = total + affine[:, a + 1 : a + 2] * fl[0, a : a + 1, :]
    total = total + affine[:, 0:1]
    order_s = list(range(S - 1, 0, -1))
    for m in order_s:
        send_motion(m).wait_recv()
        total = total + mo_in[m]
    out[0, :, 0:wf] = total
    total = ld_out[0]
    send_other().wait_recv()
    total = total + ld_in[0]
    for j in range(half - 1, 0, -1):
        send_loads(j).wait_recv()
        total = total + ld_in[j]
    out[1, :, 0:wc] = total
    for m in order_s:
        send_fluid(m).wait_send()
        send_motion(m).wait_send()
    for p in range(1, half + 1):
        send_center(p).wait_send()
    for p in range(1, half):
        hand_on(p).wait_send()
        send_pre(p + half).wait_send()
        send_loads(p).wait_send()
    send_other().wait_send()


def per_device(rows, cols, side, fluid_data, center_data, poly_coef):
    f32, bf16 = jnp.float32, jnp.bfloat16
    S, T = cols // side, rows * side
    height, wf = fluid_data.shape
    wc = center_data.shape[1]
    n = height - 3
    vmem = pl.BlockSpec(memory_space=pltpu.VMEM)
    hbm = pl.BlockSpec(memory_space=pltpu.HBM)
    sems = [pltpu.SemaphoreType.DMA((k,)) for k in (3, S, S, T, T, S, S, T // 2, T // 2, T // 2, T // 2)]
    both = pl.pallas_call(
        functools.partial(body, rows, cols, side),
        out_shape=jax.ShapeDtypeStruct((2, n, max(wf, wc)), f32),
        in_specs=[hbm] * 3,
        out_specs=vmem,
        scratch_shapes=[
            pltpu.VMEM((S, height, wf), f32),
            pltpu.VMEM((T, height, wc), f32),
            pltpu.VMEM((4, n), f32),
            pltpu.VMEM((2, DEPTH, max(wf, wc)), f32),
            pltpu.VMEM((S, wf, DEPTH), bf16),
            pltpu.VMEM((T, DEPTH, wc), bf16),
            pltpu.VMEM((T, 2 * n, wc), bf16),
            pltpu.VMEM((S, 2 * n, wf), bf16),
            pltpu.VMEM((4, wf, wc), f32),
            pltpu.VMEM((4, wf, wc), bf16),
            pltpu.VMEM((4, wf, wc), bf16),
            pltpu.VMEM((S, n, wf), f32),
            pltpu.VMEM((S, n, wf), f32),
            pltpu.VMEM((T, n, wc), f32),
            pltpu.VMEM((T // 2, n, wc), f32),
            pltpu.VMEM((T // 2, n, wc), f32),
            *sems,
        ],
        compiler_params=pltpu.CompilerParams(
            collective_id=0, has_side_effects=True, vmem_limit_bytes=67_043_328
        ),
    )(fluid_data, center_data, poly_coef.T)
    return both[0, :, :wf], both[1, :, :wc]


def solution(mesh):
    rows, cols = mesh.shape["row"], mesh.shape["col"]
    side = 2 if cols % 2 == 0 else 1
    placed = (P(None, ("row", "col")), P(None, ("col", "row")), P())
    return jax.shard_map(
        functools.partial(per_device, rows, cols, side),
        mesh=mesh,
        in_specs=placed,
        out_specs=(P(None, ("row", "col")), P(None, ("col", "row"))),
        check_vma=False,
    )
```

```python
import functools

import jax
import jax.numpy as jnp
from jax import lax
from jax.experimental import pallas as pl
from jax.experimental.pallas import tpu as pltpu
from jax.sharding import PartitionSpec as P

WAVES = 64
MESH = pl.DeviceIdType.MESH
TOP = 12.404427306735432
MID = 0.6418441597071612
LOW = 0.16126480593510223
DEPTH = 128


def paired(me, m, n):
    other, bit = 0, 1
    while bit < n:
        other = other + (((me // bit) % 2 + (m // bit) % 2) % 2) * bit
        bit *= 2
    return other


def dot(a, b, dims):
    return lax.dot_general(a, b, (dims, ((), ())), preferred_element_type=jnp.float32)


def rounded(x):
    return x.astype(jnp.bfloat16).astype(jnp.float32)


def split(x):
    high = x.astype(jnp.bfloat16)
    low = (x - high.astype(jnp.float32)).astype(jnp.bfloat16)
    return high, low


def pieces(places):
    x = places * float(WAVES)
    coarse = jnp.round(x * 2.0) * 0.5
    fine = x - coarse
    coarse = coarse - float(WAVES // 2)
    first = rounded(fine)
    second = rounded(fine - first)
    fine = first + second
    large = coarse * coarse
    small = fine * (coarse + coarse) + fine * fine
    large = large[0:1] + large[1:2] + large[2:3]
    small = small[0:1] + small[1:2] + small[2:3]
    l1 = rounded(large)
    l2 = large - l1
    s1 = rounded(small)
    s2 = rounded(small - s1)
    s3 = small - s1 - s2
    return coarse, first, second, (l1, l2), (s1, s2, s3)


def rows_of(base, at, extra):
    out = jnp.where(at < 3, base, 0.0)
    for i, e in extra:
        out = jnp.where(at == i, e, out)
    return out


def center_rows(places):
    c, f1, f2, large, small = pieces(places)
    at = lax.broadcasted_iota(jnp.int32, places.shape, 0)
    one = 1.0
    return [
        rows_of(c, at, [(3, large[0]), (4, large[1]), (5, one), (6, one)]),
        rows_of(c, at, [(3, small[0]), (4, small[1]), (5, small[2])]),
        rows_of(c, at, [(3, one), (4, one), (5, one)]),
        rows_of(f1, at, []),
        rows_of(f2, at, []),
        rows_of(f1, at, []),
        rows_of(f1, at, []),
        rows_of(f2, at, []),
        rows_of(f2, at, []),
    ]


def fluid_rows(places):
    c, f1, f2, large, small = pieces(places)
    at = lax.broadcasted_iota(jnp.int32, places.shape, 0)
    one = 1.0
    c, f1, f2 = -2.0 * c, -2.0 * f1, -2.0 * f2
    return [
        rows_of(c, at, [(3, one), (4, one), (5, large[0]), (6, large[1])]),
        rows_of(f1, at, [(3, one), (4, one), (5, one)]),
        rows_of(f2, at, [(3, small[0]), (4, small[1]), (5, small[2])]),
        rows_of(c, at, []),
        rows_of(c, at, []),
        rows_of(f1, at, []),
        rows_of(f2, at, []),
        rows_of(f1, at, []),
        rows_of(f2, at, []),
    ]


def plan_of(S, T):
    half = T // 2
    near = list(range(1, min(half, 3)))
    far = list(range(3, half))
    groups = [([("c", half)], [(0, 0), (0, half)])]
    first = [(0, p) for p in near] + [(1, 0), (1, half)]
    groups.append(([("c", p) for p in near] + [("f", 1)], first))
    more = [("c", p) for p in far[:1]] + [("c", half + p) for p in near]
    tiles = [(m, half + p) for p in near for m in (0, 1)]
    tiles += [(m, p) for p in far[:1] for m in (0, 1)]
    groups.append((more, tiles))
    for p in far[1:]:
        groups.append(([("c", p), ("c", half + p - 1)], [(0, p), (1, p), (0, half + p - 1), (1, half + p - 1)]))
    last = far[-1:]
    every = [0, half] + list(range(1, half)) + list(range(half + 1, T))
    tiles = [(m, half + p) for p in last for m in (0, 1)] + [(2, r) for r in every]
    groups.append(([("c", half + p) for p in last] + [("f", 2)], tiles))
    for m in range(S - 2, 2, -1):
        groups.append(([("f", m)], [(m, r) for r in every]))
    tiles = [(S - 1, r) for r in list(range(T - 1, half, -1)) + list(range(half - 1, 0, -1)) + [half, 0]]
    tiles += [(1, p) for p in near]
    groups.append(([("f", S - 1)], tiles))
    order, needs = [], {}
    for need, tiles in groups:
        needs[len(order) // 2] = need
        order += tiles
    assert len(set(order)) == S * T == len(order)
    return [order[i : i + 2] for i in range(0, len(order), 2)], needs


def body(rows, cols, side, fluid, center, poly, out, *scratch):
    (fl, ce, pv, fa, ff, fc, chl, fhl, sq, kh, kl, mo_out, mo_in, ld_out, ld_in, pre) = scratch[:16]
    own, fs, fr, cs, cr, ms, mr, ls, lr, ps, pr = scratch[16:]
    S, T = cols // side, rows * side
    half = T // 2
    row, col = lax.axis_index("row"), lax.axis_index("col")
    my_s, my_t = col // side, (row % 2) * half + (col % side) * (rows // 2) + row // 2
    nvals = pv.shape[1]
    wf, wc = fluid.shape[1], center.shape[1]

    def along_s(m):
        return {"row": row, "col": paired(my_s, m, S) * side + col % side}

    def along_t(m):
        i = paired(my_t, m, T)
        return {
            "row": (i % (rows // 2)) * 2 + i // half,
            "col": (col // side) * side + (i % half) // (rows // 2),
        }

    def copy(src, dst, send, recv, where):
        return pltpu.make_async_remote_copy(
            src_ref=src, dst_ref=dst, send_sem=send, recv_sem=recv, device_id=where, device_id_type=MESH
        )

    def send_fluid(m):
        return copy(fl.at[0], fl.at[m], fs.at[m], fr.at[m], along_s(m))

    def send_center(p):
        return copy(ce.at[0], ce.at[p], cs.at[p], cr.at[p], along_t(p))

    def hand_on(p):
        q = p + half
        return copy(ce.at[p], ce.at[q], cs.at[q], cr.at[q], along_t(half))

    def send_motion(m):
        return copy(mo_out.at[m], mo_in.at[m], ms.at[m], mr.at[m], along_s(m))

    def send_pre(p):
        j = p - half
        return copy(ld_out.at[p], pre.at[j], ps.at[j], pr.at[j], along_t(half))

    def send_loads(j):
        return copy(ld_out.at[j], ld_in.at[j], ls.at[j], lr.at[j], along_t(j))

    def send_other():
        return copy(ld_out.at[half], ld_in.at[0], ls.at[0], lr.at[0], along_t(half))

    local = [
        pltpu.make_async_copy(center, ce.at[0], own.at[0]),
        pltpu.make_async_copy(fluid, fl.at[0], own.at[1]),
        pltpu.make_async_copy(poly, pv, own.at[2]),
    ]
    for c in local:
        c.start()
    barrier = pltpu.get_barrier_semaphore()
    for p in range(1, half + 1):
        pl.semaphore_signal(barrier, inc=1, device_id=along_t(p), device_id_type=MESH)
    for m in range(1, S):
        pl.semaphore_signal(barrier, inc=1, device_id=along_s(m), device_id_type=MESH)
    fc[...] = jnp.zeros(fc.shape, jnp.bfloat16)
    fa[...] = jnp.zeros(fa.shape, jnp.float32)
    for c in local:
        c.wait()
    pl.semaphore_wait(barrier, S - 1 + half)
    for p in [half] + list(range(1, half)):
        send_center(p).start()
    for m in [1] + list(range(2, S)):
        send_fluid(m).start()

    def ready_center(r):
        for g, x in enumerate(center_rows(ce[r, 0:8, :])):
            fa[0, 8 * g : 8 * g + 8, 0:wc] = x
        depth = 8 * 9
        fc[r, 0 : depth + 8, :] = fa[0, 0 : depth + 8, 0:wc].astype(jnp.bfloat16)
        high, low = split(ce[r, 3:, :] * TOP)
        chl[r, 0:nvals] = high
        chl[r, nvals:] = low

    def ready_fluid(m):
        for g, x in enumerate(fluid_rows(fl[m, 0:8, :])):
            fa[1, 8 * g : 8 * g + 8, 0:wf] = x
        ff[m] = jnp.transpose(fa[1, :, 0:wf]).astype(jnp.bfloat16)
        high, low = split(fl[m, 3:, :] * TOP)
        fhl[m, 0:nvals] = high
        fhl[m, nvals:] = low

    def squares(tile, slot):
        m, r = tile
        sq[slot] = dot(ff[m], fc[r], ((1,), (0,)))

    def values(slot):
        step = 32 if wf % 32 == 0 else wf
        for j in range(0, wf, step):
            at = pl.ds(j, step)
            s = sq[slot, at, :]
            inv = lax.rsqrt(s)
            turns = s * inv
            f = turns - jnp.round(turns)
            size = jnp.abs(f)
            rest = 0.5 - size
            q = size * rest
            value = (f * rest * inv) * ((q + MID) * q + LOW)
            high, low = split(value)
            kh[slot, at, :] = high
            kl[slot, at, :] = low

    seen = set()

    def add(ref, i, name, x):
        if (name, i) in seen:
            ref[i] += x
        else:
            ref[i] = x
            seen.add((name, i))

    def sums(tile, slot):
        m, r = tile
        k_high, k_low = kh[slot], kl[slot]
        across = ((1,), (0,))
        wide = dot(fhl[m], k_high, across)
        add(ld_out, r, "l", wide[:nvals] + wide[nvals:] + dot(fhl[m, 0:nvals], k_low, across))
        back = ((1,), (1,))
        wide = dot(chl[r], k_high, back)
        add(mo_out, m, "m", wide[:nvals] + wide[nvals:] + dot(chl[r, 0:nvals], k_low, back))

    pairs, needs = plan_of(S, T)
    handed = {0}
    left_m = {m: T for m in range(S)}
    left_r = {r: S for r in range(T)}
    waiting, sent_at = [], {}
    ready_fluid(0)
    ready_center(0)

    def receive(r):
        if r <= half and r not in handed:
            send_center(r).wait_recv()
            if r < half:
                hand_on(r).start()
            handed.add(r)

    def fetch(k):
        fresh = []
        for kind, i in needs.get(k, []):
            if kind == "f":
                send_fluid(i).wait_recv()
                fresh.append((ready_fluid, i))
            else:
                if i <= half:
                    receive(i)
                else:
                    hand_on(i - half).wait_recv()
                fresh.append((ready_center, i))
        return fresh

    def finish(j):
        send_pre(half + j).wait_recv()
        ld_out[j] += pre[j]
        send_loads(j).start()

    def done(pair, k):
        for m, r in pair:
            left_m[m] -= 1
            left_r[r] -= 1
            if m and not left_m[m]:
                send_motion(m).start()
            if r and not left_r[r]:
                if r > half:
                    send_pre(r).start()
                    sent_at[r] = k
                elif r == half:
                    send_other().start()
                else:
                    waiting.append(r)

    slot_of = lambda k, i: (k % 2) * 2 + i
    for f, i in fetch(0):
        f(i)
    for i in range(2):
        squares(pairs[0][i], slot_of(0, i))
    for i in range(2):
        values(slot_of(0, i))
    n = len(pairs)
    for k in range(n + 1):
        fresh = fetch(k + 1) if k + 1 < n else []
        for i in range(2):
            if k > 1:
                sums(pairs[k - 1][i], slot_of(k - 1, i))
            if k == 0:
                sums(pairs[0][i], slot_of(0, i))
        for f, i in fresh:
            f(i)
        for i in range(2):
            if k + 1 < n:
                squares(pairs[k + 1][i], slot_of(k + 1, i))
        for i in range(2):
            if 0 < k < n:
                values(slot_of(k, i))
        if k > 0:
            done(pairs[k - 1], k)
            for j in list(waiting):
                if k >= sent_at.get(half + j, n) + 2 or k == n:
                    finish(j)
                    waiting.remove(j)

    total = mo_out[0]
    affine = jnp.transpose(pv[...])
    for a in range(3):
        total = total + affine[:, a + 1 : a + 2] * fl[0, a : a + 1, :]
    total = total + affine[:, 0:1]
    order_s = list(range(S - 1, 0, -1))
    for m in order_s:
        send_motion(m).wait_recv()
        total = total + mo_in[m]
    out[0, :, 0:wf] = total
    total = ld_out[0]
    send_other().wait_recv()
    total = total + ld_in[0]
    for j in range(half - 1, 0, -1):
        send_loads(j).wait_recv()
        total = total + ld_in[j]
    out[1, :, 0:wc] = total
    for m in order_s:
        send_fluid(m).wait_send()
        send_motion(m).wait_send()
    for p in range(1, half + 1):
        send_center(p).wait_send()
    for p in range(1, half):
        hand_on(p).wait_send()
        send_pre(p + half).wait_send()
        send_loads(p).wait_send()
    send_other().wait_send()


def per_device(rows, cols, side, fluid_data, center_data, poly_coef):
    f32, bf16 = jnp.float32, jnp.bfloat16
    S, T = cols // side, rows * side
    height, wf = fluid_data.shape
    wc = center_data.shape[1]
    n = height - 3
    vmem = pl.BlockSpec(memory_space=pltpu.VMEM)
    hbm = pl.BlockSpec(memory_space=pltpu.HBM)
    sems = [pltpu.SemaphoreType.DMA((k,)) for k in (3, S, S, T, T, S, S, T // 2, T // 2, T // 2, T // 2)]
    both = pl.pallas_call(
        functools.partial(body, rows, cols, side),
        out_shape=jax.ShapeDtypeStruct((2, n, max(wf, wc)), f32),
        in_specs=[hbm] * 3,
        out_specs=vmem,
        scratch_shapes=[
            pltpu.VMEM((S, height, wf), f32),
            pltpu.VMEM((T, height, wc), f32),
            pltpu.VMEM((4, n), f32),
            pltpu.VMEM((2, DEPTH, max(wf, wc)), f32),
            pltpu.VMEM((S, wf, DEPTH), bf16),
            pltpu.VMEM((T, DEPTH, wc), bf16),
            pltpu.VMEM((T, 2 * n, wc), bf16),
            pltpu.VMEM((S, 2 * n, wf), bf16),
            pltpu.VMEM((4, wf, wc), f32),
            pltpu.VMEM((4, wf, wc), bf16),
            pltpu.VMEM((4, wf, wc), bf16),
            pltpu.VMEM((S, n, wf), f32),
            pltpu.VMEM((S, n, wf), f32),
            pltpu.VMEM((T, n, wc), f32),
            pltpu.VMEM((T // 2, n, wc), f32),
            pltpu.VMEM((T // 2, n, wc), f32),
            *sems,
        ],
        compiler_params=pltpu.CompilerParams(
            collective_id=0, has_side_effects=True, vmem_limit_bytes=67_043_328
        ),
    )(fluid_data, center_data, poly_coef.T)
    return both[0, :, :wf], both[1, :, :wc]


def solution(mesh):
    rows, cols = mesh.shape["row"], mesh.shape["col"]
    side = 2 if cols % 2 == 0 else 1
    placed = (P(None, ("row", "col")), P(None, ("col", "row")), P())
    return jax.shard_map(
        functools.partial(per_device, rows, cols, side),
        mesh=mesh,
        in_specs=placed,
        out_specs=(P(None, ("row", "col")), P(None, ("col", "row"))),
        check_vma=False,
    )
```

```python
import functools

import jax
import jax.numpy as jnp
from jax import lax
from jax.experimental import pallas as pl
from jax.experimental.pallas import tpu as pltpu
from jax.sharding import PartitionSpec as P

WAVES = 64
MESH = pl.DeviceIdType.MESH
TOP = 12.404427306735432
MID = 0.6418441597071612
LOW = 0.16126480593510223
DEPTH = 128


def paired(me, m, n):
    other, bit = 0, 1
    while bit < n:
        other = other + (((me // bit) % 2 + (m // bit) % 2) % 2) * bit
        bit *= 2
    return other


def dot(a, b, dims):
    return lax.dot_general(a, b, (dims, ((), ())), preferred_element_type=jnp.float32)


def rounded(x):
    return x.astype(jnp.bfloat16).astype(jnp.float32)


def split(x):
    high = x.astype(jnp.bfloat16)
    low = (x - high.astype(jnp.float32)).astype(jnp.bfloat16)
    return high, low


def pieces(places):
    x = places * float(WAVES)
    coarse = jnp.round(x * 2.0) * 0.5
    fine = x - coarse
    coarse = coarse - float(WAVES // 2)
    first = rounded(fine)
    second = rounded(fine - first)
    fine = first + second
    large = coarse * coarse
    small = fine * (coarse + coarse) + fine * fine
    large = large[0:1] + large[1:2] + large[2:3]
    small = small[0:1] + small[1:2] + small[2:3]
    l1 = rounded(large)
    l2 = large - l1
    s1 = rounded(small)
    s2 = rounded(small - s1)
    s3 = small - s1 - s2
    return coarse, first, second, (l1, l2), (s1, s2, s3)


def rows_of(base, at, extra):
    out = jnp.where(at < 3, base, 0.0)
    for i, e in extra:
        out = jnp.where(at == i, e, out)
    return out


def center_rows(places):
    c, f1, f2, large, small = pieces(places)
    at = lax.broadcasted_iota(jnp.int32, places.shape, 0)
    one = 1.0
    return [
        rows_of(c, at, [(3, large[0]), (4, large[1]), (5, one), (6, one)]),
        rows_of(c, at, [(3, small[0]), (4, small[1]), (5, small[2])]),
        rows_of(c, at, [(3, one), (4, one), (5, one)]),
        rows_of(f1, at, []),
        rows_of(f2, at, []),
        rows_of(f1, at, []),
        rows_of(f1, at, []),
        rows_of(f2, at, []),
        rows_of(f2, at, []),
    ]


def fluid_rows(places):
    c, f1, f2, large, small = pieces(places)
    at = lax.broadcasted_iota(jnp.int32, places.shape, 0)
    one = 1.0
    c, f1, f2 = -2.0 * c, -2.0 * f1, -2.0 * f2
    return [
        rows_of(c, at, [(3, one), (4, one), (5, large[0]), (6, large[1])]),
        rows_of(f1, at, [(3, one), (4, one), (5, one)]),
        rows_of(f2, at, [(3, small[0]), (4, small[1]), (5, small[2])]),
        rows_of(c, at, []),
        rows_of(c, at, []),
        rows_of(f1, at, []),
        rows_of(f2, at, []),
        rows_of(f1, at, []),
        rows_of(f2, at, []),
    ]


def plan_of(S, T):
    half = T // 2
    near = list(range(1, min(half, 3)))
    far = list(range(3, half))
    groups = [([("c", half)], [(0, 0), (0, half)])]
    first = [(0, p) for p in near] + [(1, 0), (1, half)]
    groups.append(([("c", p) for p in near] + [("f", 1)], first))
    more = [("c", p) for p in far[:1]] + [("c", half + p) for p in near]
    tiles = [(m, half + p) for p in near for m in (0, 1)]
    tiles += [(m, p) for p in far[:1] for m in (0, 1)]
    groups.append((more, tiles))
    for p in far[1:]:
        groups.append(([("c", p), ("c", half + p - 1)], [(0, p), (1, p), (0, half + p - 1), (1, half + p - 1)]))
    last = far[-1:]
    every = [0, half] + list(range(1, half)) + list(range(half + 1, T))
    tiles = [(m, half + p) for p in last for m in (0, 1)] + [(2, r) for r in every]
    groups.append(([("c", half + p) for p in last] + [("f", 2)], tiles))
    for m in range(S - 2, 2, -1):
        groups.append(([("f", m)], [(m, r) for r in every]))
    tiles = [(S - 1, r) for r in list(range(T - 1, half, -1)) + list(range(half - 1, 0, -1)) + [half, 0]]
    tiles += [(1, p) for p in near]
    groups.append(([("f", S - 1)], tiles))
    order, needs = [], {}
    for need, tiles in groups:
        needs[len(order) // 2] = need
        order += tiles
    assert len(set(order)) == S * T == len(order)
    return [order[i : i + 2] for i in range(0, len(order), 2)], needs


def body(rows, cols, side, fluid, center, poly, out, *scratch):
    (fl, ce, pv, fa, ff, fc, chl, fhl, sq, kh, kl, mo_out, mo_in, ld_out, ld_in, pre) = scratch[:16]
    own, fs, fr, cs, cr, ms, mr, ls, lr, ps, pr = scratch[16:]
    S, T = cols // side, rows * side
    half = T // 2
    row, col = lax.axis_index("row"), lax.axis_index("col")
    my_s, my_t = col // side, (row % 2) * half + (col % side) * (rows // 2) + row // 2
    nvals = pv.shape[1]
    wf, wc = fluid.shape[1], center.shape[1]

    def along_s(m):
        return {"row": row, "col": paired(my_s, m, S) * side + col % side}

    def along_t(m):
        i = paired(my_t, m, T)
        return {
            "row": (i % (rows // 2)) * 2 + i // half,
            "col": (col // side) * side + (i % half) // (rows // 2),
        }

    def copy(src, dst, send, recv, where):
        return pltpu.make_async_remote_copy(
            src_ref=src, dst_ref=dst, send_sem=send, recv_sem=recv, device_id=where, device_id_type=MESH
        )

    def send_fluid(m):
        return copy(fl.at[0], fl.at[m], fs.at[m], fr.at[m], along_s(m))

    def send_center(p):
        return copy(ce.at[0], ce.at[p], cs.at[p], cr.at[p], along_t(p))

    def hand_on(p):
        q = p + half
        return copy(ce.at[p], ce.at[q], cs.at[q], cr.at[q], along_t(half))

    def send_motion(m):
        return copy(mo_out.at[m], mo_in.at[m], ms.at[m], mr.at[m], along_s(m))

    def send_pre(p):
        j = p - half
        return copy(ld_out.at[p], pre.at[j], ps.at[j], pr.at[j], along_t(half))

    def send_loads(j):
        return copy(ld_out.at[j], ld_in.at[j], ls.at[j], lr.at[j], along_t(j))

    def send_other():
        return copy(ld_out.at[half], ld_in.at[0], ls.at[0], lr.at[0], along_t(half))

    local = [
        pltpu.make_async_copy(center, ce.at[0], own.at[0]),
        pltpu.make_async_copy(fluid, fl.at[0], own.at[1]),
        pltpu.make_async_copy(poly, pv, own.at[2]),
    ]
    for c in local:
        c.start()
    barrier = pltpu.get_barrier_semaphore()
    for p in range(1, half + 1):
        pl.semaphore_signal(barrier, inc=1, device_id=along_t(p), device_id_type=MESH)
    for m in range(1, S):
        pl.semaphore_signal(barrier, inc=1, device_id=along_s(m), device_id_type=MESH)
    fc[...] = jnp.zeros(fc.shape, jnp.bfloat16)
    fa[...] = jnp.zeros(fa.shape, jnp.float32)
    for c in local:
        c.wait()
    pl.semaphore_wait(barrier, S - 1 + half)
    for p in [half] + list(range(1, half)):
        send_center(p).start()
    for m in [1] + list(range(2, S)):
        send_fluid(m).start()

    def ready_center(r):
        for g, x in enumerate(center_rows(ce[r, 0:8, :])):
            fa[0, 8 * g : 8 * g + 8, 0:wc] = x
        depth = 8 * 9
        fc[r, 0 : depth + 8, :] = fa[0, 0 : depth + 8, 0:wc].astype(jnp.bfloat16)
        high, low = split(ce[r, 3:, :] * TOP)
        chl[r, 0:nvals] = high
        chl[r, nvals:] = low

    def ready_fluid(m):
        for g, x in enumerate(fluid_rows(fl[m, 0:8, :])):
            fa[1, 8 * g : 8 * g + 8, 0:wf] = x
        ff[m] = jnp.transpose(fa[1, :, 0:wf]).astype(jnp.bfloat16)
        high, low = split(fl[m, 3:, :] * TOP)
        fhl[m, 0:nvals] = high
        fhl[m, nvals:] = low

    def squares(tile, slot):
        m, r = tile
        sq[slot] = dot(ff[m], fc[r], ((1,), (0,)))

    def values(slot):
        step = 32 if wf % 32 == 0 else wf
        for j in range(0, wf, step):
            at = pl.ds(j, step)
            s = sq[slot, at, :]
            inv = lax.rsqrt(s)
            turns = s * inv
            f = turns - jnp.round(turns)
            size = jnp.abs(f)
            rest = 0.5 - size
            q = size * rest
            value = (f * rest * inv) * ((q + MID) * q + LOW)
            high, low = split(value)
            kh[slot, at, :] = high
            kl[slot, at, :] = low

    seen = set()

    def add(ref, i, name, x):
        if (name, i) in seen:
            ref[i] += x
        else:
            ref[i] = x
            seen.add((name, i))

    def sums(tile, slot):
        m, r = tile
        k_high, k_low = kh[slot], kl[slot]
        across = ((1,), (0,))
        wide = dot(fhl[m], k_high, across)
        add(ld_out, r, "l", wide[:nvals] + wide[nvals:] + dot(fhl[m, 0:nvals], k_low, across))
        back = ((1,), (1,))
        wide = dot(chl[r], k_high, back)
        add(mo_out, m, "m", wide[:nvals] + wide[nvals:] + dot(chl[r, 0:nvals], k_low, back))

    pairs, needs = plan_of(S, T)
    handed = {0}
    left_m = {m: T for m in range(S)}
    left_r = {r: S for r in range(T)}
    waiting, sent_at = [], {}
    ready_fluid(0)
    ready_center(0)

    def receive(r):
        if r <= half and r not in handed:
            send_center(r).wait_recv()
            if r < half:
                hand_on(r).start()
            handed.add(r)

    def fetch(k):
        fresh = []
        for kind, i in needs.get(k, []):
            if kind == "f":
                send_fluid(i).wait_recv()
                fresh.append((ready_fluid, i))
            else:
                if i <= half:
                    receive(i)
                else:
                    hand_on(i - half).wait_recv()
                fresh.append((ready_center, i))
        return fresh

    def finish(j):
        send_pre(half + j).wait_recv()
        ld_out[j] += pre[j]
        send_loads(j).start()

    def done(pair, k):
        for m, r in pair:
            left_m[m] -= 1
            left_r[r] -= 1
            if m and not left_m[m]:
                send_motion(m).start()
            if r and not left_r[r]:
                if r > half:
                    send_pre(r).start()
                    sent_at[r] = k
                elif r == half:
                    send_other().start()
                else:
                    waiting.append(r)

    slot_of = lambda k, i: (k % 2) * 2 + i
    for f, i in fetch(0):
        f(i)
    for i in range(2):
        squares(pairs[0][i], slot_of(0, i))
    for i in range(2):
        values(slot_of(0, i))
    for i in range(2):
        sums(pairs[0][i], slot_of(0, i))
    n = len(pairs)
    for k in range(n + 1):
        fresh = fetch(k + 1) if k + 1 < n else []
        for i in range(2):
            if k > 1:
                sums(pairs[k - 1][i], slot_of(k - 1, i))
        for f, i in fresh:
            f(i)
        for i in range(2):
            if k + 1 < n:
                squares(pairs[k + 1][i], slot_of(k + 1, i))
        for i in range(2):
            if 0 < k < n:
                values(slot_of(k, i))
        if k > 0:
            done(pairs[k - 1], k)
            for j in list(waiting):
                if k >= sent_at.get(half + j, n) + 2 or k == n:
                    finish(j)
                    waiting.remove(j)

    total = mo_out[0]
    affine = jnp.transpose(pv[...])
    for a in range(3):
        total = total + affine[:, a + 1 : a + 2] * fl[0, a : a + 1, :]
    total = total + affine[:, 0:1]
    order_s = list(range(S - 1, 0, -1))
    for m in order_s:
        send_motion(m).wait_recv()
        total = total + mo_in[m]
    out[0, :, 0:wf] = total
    total = ld_out[0]
    send_other().wait_recv()
    total = total + ld_in[0]
    for j in range(half - 1, 0, -1):
        send_loads(j).wait_recv()
        total = total + ld_in[j]
    out[1, :, 0:wc] = total
    for m in order_s:
        send_fluid(m).wait_send()
        send_motion(m).wait_send()
    for p in range(1, half + 1):
        send_center(p).wait_send()
    for p in range(1, half):
        hand_on(p).wait_send()
        send_pre(p + half).wait_send()
        send_loads(p).wait_send()
    send_other().wait_send()


def per_device(rows, cols, side, fluid_data, center_data, poly_coef):
    f32, bf16 = jnp.float32, jnp.bfloat16
    S, T = cols // side, rows * side
    height, wf = fluid_data.shape
    wc = center_data.shape[1]
    n = height - 3
    vmem = pl.BlockSpec(memory_space=pltpu.VMEM)
    hbm = pl.BlockSpec(memory_space=pltpu.HBM)
    sems = [pltpu.SemaphoreType.DMA((k,)) for k in (3, S, S, T, T, S, S, T // 2, T // 2, T // 2, T // 2)]
    both = pl.pallas_call(
        functools.partial(body, rows, cols, side),
        out_shape=jax.ShapeDtypeStruct((2, n, max(wf, wc)), f32),
        in_specs=[hbm] * 3,
        out_specs=vmem,
        scratch_shapes=[
            pltpu.VMEM((S, height, wf), f32),
            pltpu.VMEM((T, height, wc), f32),
            pltpu.VMEM((4, n), f32),
            pltpu.VMEM((2, DEPTH, max(wf, wc)), f32),
            pltpu.VMEM((S, wf, DEPTH), bf16),
            pltpu.VMEM((T, DEPTH, wc), bf16),
            pltpu.VMEM((T, 2 * n, wc), bf16),
            pltpu.VMEM((S, 2 * n, wf), bf16),
            pltpu.VMEM((4, wf, wc), f32),
            pltpu.VMEM((4, wf, wc), bf16),
            pltpu.VMEM((4, wf, wc), bf16),
            pltpu.VMEM((S, n, wf), f32),
            pltpu.VMEM((S, n, wf), f32),
            pltpu.VMEM((T, n, wc), f32),
            pltpu.VMEM((T // 2, n, wc), f32),
            pltpu.VMEM((T // 2, n, wc), f32),
            *sems,
        ],
        compiler_params=pltpu.CompilerParams(
            collective_id=0, has_side_effects=True, vmem_limit_bytes=67_043_328
        ),
    )(fluid_data, center_data, poly_coef.T)
    return both[0, :, :wf], both[1, :, :wc]


def solution(mesh):
    rows, cols = mesh.shape["row"], mesh.shape["col"]
    side = 2 if cols % 2 == 0 else 1
    placed = (P(None, ("row", "col")), P(None, ("col", "row")), P())
    return jax.shard_map(
        functools.partial(per_device, rows, cols, side),
        mesh=mesh,
        in_specs=placed,
        out_specs=(P(None, ("row", "col")), P(None, ("col", "row"))),
        check_vma=False,
    )
```

```python
import functools

import jax
import jax.numpy as jnp
from jax import lax
from jax.experimental import pallas as pl
from jax.experimental.pallas import tpu as pltpu
from jax.sharding import PartitionSpec as P

WAVES = 64
MESH = pl.DeviceIdType.MESH
TOP = 12.404427306735432
MID = 0.6418441597071612
LOW = 0.16126480593510223
DEPTH = 128


def paired(me, m, n):
    other, bit = 0, 1
    while bit < n:
        other = other + (((me // bit) % 2 + (m // bit) % 2) % 2) * bit
        bit *= 2
    return other


def dot(a, b, dims):
    return lax.dot_general(a, b, (dims, ((), ())), preferred_element_type=jnp.float32)


def rounded(x):
    return x.astype(jnp.bfloat16).astype(jnp.float32)


def split(x):
    high = x.astype(jnp.bfloat16)
    low = (x - high.astype(jnp.float32)).astype(jnp.bfloat16)
    return high, low


def pieces(places):
    x = places * float(WAVES)
    coarse = jnp.round(x * 2.0) * 0.5
    fine = x - coarse
    coarse = coarse - float(WAVES // 2)
    first = rounded(fine)
    second = rounded(fine - first)
    fine = first + second
    large = coarse * coarse
    small = fine * (coarse + coarse) + fine * fine
    large = large[0:1] + large[1:2] + large[2:3]
    small = small[0:1] + small[1:2] + small[2:3]
    l1 = rounded(large)
    l2 = large - l1
    s1 = rounded(small)
    s2 = rounded(small - s1)
    s3 = small - s1 - s2
    return coarse, first, second, (l1, l2), (s1, s2, s3)


def rows_of(base, at, extra):
    out = jnp.where(at < 3, base, 0.0)
    for i, e in extra:
        out = jnp.where(at == i, e, out)
    return out


def center_rows(places):
    c, f1, f2, large, small = pieces(places)
    at = lax.broadcasted_iota(jnp.int32, places.shape, 0)
    one = 1.0
    return [
        rows_of(c, at, [(3, large[0]), (4, large[1]), (5, one), (6, one)]),
        rows_of(c, at, [(3, small[0]), (4, small[1]), (5, small[2])]),
        rows_of(c, at, [(3, one), (4, one), (5, one)]),
        rows_of(f1, at, []),
        rows_of(f2, at, []),
        rows_of(f1, at, []),
        rows_of(f1, at, []),
        rows_of(f2, at, []),
        rows_of(f2, at, []),
    ]


def fluid_rows(places):
    c, f1, f2, large, small = pieces(places)
    at = lax.broadcasted_iota(jnp.int32, places.shape, 0)
    one = 1.0
    c, f1, f2 = -2.0 * c, -2.0 * f1, -2.0 * f2
    return [
        rows_of(c, at, [(3, one), (4, one), (5, large[0]), (6, large[1])]),
        rows_of(f1, at, [(3, one), (4, one), (5, one)]),
        rows_of(f2, at, [(3, small[0]), (4, small[1]), (5, small[2])]),
        rows_of(c, at, []),
        rows_of(c, at, []),
        rows_of(f1, at, []),
        rows_of(f2, at, []),
        rows_of(f1, at, []),
        rows_of(f2, at, []),
    ]


def plan_of(S, T):
    half = T // 2
    near = list(range(1, min(half, 3)))
    far = list(range(3, half))
    groups = [([("c", half)], [(0, 0), (0, half)])]
    first = [(0, p) for p in near] + [(1, 0), (1, half)]
    groups.append(([("c", p) for p in near] + [("f", 1)], first))
    more = [("c", p) for p in far[:1]] + [("c", half + p) for p in near]
    tiles = [(m, half + p) for p in near for m in (0, 1)]
    tiles += [(m, p) for p in far[:1] for m in (0, 1)]
    groups.append((more, tiles))
    for p in far[1:]:
        groups.append(([("c", p), ("c", half + p - 1)], [(0, p), (1, p), (0, half + p - 1), (1, half + p - 1)]))
    last = far[-1:]
    every = [0, half] + list(range(1, half)) + list(range(half + 1, T))
    tiles = [(m, half + p) for p in last for m in (0, 1)] + [(2, r) for r in every]
    groups.append(([("c", half + p) for p in last] + [("f", 2)], tiles))
    for m in range(S - 2, 2, -1):
        groups.append(([("f", m)], [(m, r) for r in every]))
    tiles = [(S - 1, r) for r in list(range(T - 1, half, -1)) + list(range(half - 1, 0, -1)) + [half, 0]]
    tiles += [(1, p) for p in near]
    groups.append(([("f", S - 1)], tiles))
    order, needs = [], {}
    for need, tiles in groups:
        needs[len(order) // 2] = need
        order += tiles
    assert len(set(order)) == S * T == len(order)
    return [order[i : i + 2] for i in range(0, len(order), 2)], needs


def body(rows, cols, side, fluid, center, poly, out, *scratch):
    (fl, ce, pv, fa, ff, fc, chl, fhl, sq, kh, kl, mo_out, mo_in, ld_out, ld_in, pre) = scratch[:16]
    own, fs, fr, cs, cr, ms, mr, ls, lr, ps, pr = scratch[16:]
    S, T = cols // side, rows * side
    half = T // 2
    row, col = lax.axis_index("row"), lax.axis_index("col")
    my_s, my_t = col // side, (row % 2) * half + (col % side) * (rows // 2) + row // 2
    nvals = pv.shape[1]
    wf, wc = fluid.shape[1], center.shape[1]

    def along_s(m):
        return {"row": row, "col": paired(my_s, m, S) * side + col % side}

    def along_t(m):
        i = paired(my_t, m, T)
        return {
            "row": (i % (rows // 2)) * 2 + i // half,
            "col": (col // side) * side + (i % half) // (rows // 2),
        }

    def copy(src, dst, send, recv, where):
        return pltpu.make_async_remote_copy(
            src_ref=src, dst_ref=dst, send_sem=send, recv_sem=recv, device_id=where, device_id_type=MESH
        )

    def send_fluid(m):
        return copy(fl.at[0], fl.at[m], fs.at[m], fr.at[m], along_s(m))

    def send_center(p):
        return copy(ce.at[0], ce.at[p], cs.at[p], cr.at[p], along_t(p))

    def hand_on(p):
        q = p + half
        return copy(ce.at[p], ce.at[q], cs.at[q], cr.at[q], along_t(half))

    def send_motion(m):
        return copy(mo_out.at[m], mo_in.at[m], ms.at[m], mr.at[m], along_s(m))

    def send_pre(p):
        j = p - half
        return copy(ld_out.at[p], pre.at[j], ps.at[j], pr.at[j], along_t(half))

    def send_loads(j):
        return copy(ld_out.at[j], ld_in.at[j], ls.at[j], lr.at[j], along_t(j))

    def send_other():
        return copy(ld_out.at[half], ld_in.at[0], ls.at[0], lr.at[0], along_t(half))

    local = [
        pltpu.make_async_copy(center, ce.at[0], own.at[0]),
        pltpu.make_async_copy(fluid, fl.at[0], own.at[1]),
        pltpu.make_async_copy(poly, pv, own.at[2]),
    ]
    for c in local:
        c.start()
    barrier = pltpu.get_barrier_semaphore()
    for p in range(1, half + 1):
        pl.semaphore_signal(barrier, inc=1, device_id=along_t(p), device_id_type=MESH)
    for m in range(1, S):
        pl.semaphore_signal(barrier, inc=1, device_id=along_s(m), device_id_type=MESH)
    fc[...] = jnp.zeros(fc.shape, jnp.bfloat16)
    fa[...] = jnp.zeros(fa.shape, jnp.float32)
    for c in local:
        c.wait()
    pl.semaphore_wait(barrier, S - 1 + half)
    for p in [half] + list(range(1, half)):
        send_center(p).start()
    for m in [1] + list(range(2, S)):
        send_fluid(m).start()

    def ready_center(r):
        for g, x in enumerate(center_rows(ce[r, 0:8, :])):
            fa[0, 8 * g : 8 * g + 8, 0:wc] = x
        depth = 8 * 9
        fc[r, 0 : depth + 8, :] = fa[0, 0 : depth + 8, 0:wc].astype(jnp.bfloat16)

    def values_center(r):
        high, low = split(ce[r, 3:, :] * TOP)
        chl[r, 0:nvals] = high
        chl[r, nvals:] = low

    def ready_fluid(m):
        for g, x in enumerate(fluid_rows(fl[m, 0:8, :])):
            fa[1, 8 * g : 8 * g + 8, 0:wf] = x
        ff[m] = jnp.transpose(fa[1, :, 0:wf]).astype(jnp.bfloat16)

    def values_fluid(m):
        high, low = split(fl[m, 3:, :] * TOP)
        fhl[m, 0:nvals] = high
        fhl[m, nvals:] = low

    def squares(tile, slot):
        m, r = tile
        sq[slot] = dot(ff[m], fc[r], ((1,), (0,)))

    def values(slot):
        step = 32 if wf % 32 == 0 else wf
        for j in range(0, wf, step):
            at = pl.ds(j, step)
            s = sq[slot, at, :]
            inv = lax.rsqrt(s)
            turns = s * inv
            f = turns - jnp.round(turns)
            size = jnp.abs(f)
            rest = 0.5 - size
            q = size * rest
            value = (f * rest * inv) * ((q + MID) * q + LOW)
            high, low = split(value)
            kh[slot, at, :] = high
            kl[slot, at, :] = low

    seen = set()

    def add(ref, i, name, x):
        if (name, i) in seen:
            ref[i] += x
        else:
            ref[i] = x
            seen.add((name, i))

    def sums(tile, slot):
        m, r = tile
        k_high, k_low = kh[slot], kl[slot]
        across = ((1,), (0,))
        wide = dot(fhl[m], k_high, across)
        add(ld_out, r, "l", wide[:nvals] + wide[nvals:] + dot(fhl[m, 0:nvals], k_low, across))
        back = ((1,), (1,))
        wide = dot(chl[r], k_high, back)
        add(mo_out, m, "m", wide[:nvals] + wide[nvals:] + dot(chl[r, 0:nvals], k_low, back))

    pairs, needs = plan_of(S, T)
    handed = {0}
    left_m = {m: T for m in range(S)}
    left_r = {r: S for r in range(T)}
    waiting, sent_at = [], {}
    ready_fluid(0)
    ready_center(0)
    values_fluid(0)
    values_center(0)

    def receive(r):
        if r <= half and r not in handed:
            send_center(r).wait_recv()
            if r < half:
                hand_on(r).start()
            handed.add(r)

    def fetch(k):
        fresh = []
        for kind, i in needs.get(k, []):
            if kind == "f":
                send_fluid(i).wait_recv()
                fresh.append((ready_fluid, i))
            else:
                if i <= half:
                    receive(i)
                else:
                    hand_on(i - half).wait_recv()
                fresh.append((ready_center, i))
        return fresh

    def finish(j):
        send_pre(half + j).wait_recv()
        ld_out[j] += pre[j]
        send_loads(j).start()

    def done(pair, k):
        for m, r in pair:
            left_m[m] -= 1
            left_r[r] -= 1
            if m and not left_m[m]:
                send_motion(m).start()
            if r and not left_r[r]:
                if r > half:
                    send_pre(r).start()
                    sent_at[r] = k
                elif r == half:
                    send_other().start()
                else:
                    waiting.append(r)

    slot_of = lambda k, i: (k % 2) * 2 + i
    for f, i in fetch(0):
        f(i)
        values_center(i)
    for i in range(2):
        squares(pairs[0][i], slot_of(0, i))
    for i in range(2):
        values(slot_of(0, i))
    for i in range(2):
        sums(pairs[0][i], slot_of(0, i))
    n = len(pairs)
    for k in range(n + 1):
        fresh = fetch(k + 1) if k + 1 < n else []
        for i in range(2):
            if k > 1:
                sums(pairs[k - 1][i], slot_of(k - 1, i))
        for f, i in fresh:
            f(i)
        for i in range(2):
            if k + 1 < n:
                squares(pairs[k + 1][i], slot_of(k + 1, i))
        for f, i in fresh:
            (values_center if f is ready_center else values_fluid)(i)
        for i in range(2):
            if 0 < k < n:
                values(slot_of(k, i))
        if k > 0:
            done(pairs[k - 1], k)
            for j in list(waiting):
                if k >= sent_at.get(half + j, n) + 2 or k == n:
                    finish(j)
                    waiting.remove(j)

    total = mo_out[0]
    affine = jnp.transpose(pv[...])
    for a in range(3):
        total = total + affine[:, a + 1 : a + 2] * fl[0, a : a + 1, :]
    total = total + affine[:, 0:1]
    order_s = list(range(S - 1, 0, -1))
    for m in order_s:
        send_motion(m).wait_recv()
        total = total + mo_in[m]
    out[0, :, 0:wf] = total
    total = ld_out[0]
    send_other().wait_recv()
    total = total + ld_in[0]
    for j in range(half - 1, 0, -1):
        send_loads(j).wait_recv()
        total = total + ld_in[j]
    out[1, :, 0:wc] = total
    for m in order_s:
        send_fluid(m).wait_send()
        send_motion(m).wait_send()
    for p in range(1, half + 1):
        send_center(p).wait_send()
    for p in range(1, half):
        hand_on(p).wait_send()
        send_pre(p + half).wait_send()
        send_loads(p).wait_send()
    send_other().wait_send()


def per_device(rows, cols, side, fluid_data, center_data, poly_coef):
    f32, bf16 = jnp.float32, jnp.bfloat16
    S, T = cols // side, rows * side
    height, wf = fluid_data.shape
    wc = center_data.shape[1]
    n = height - 3
    vmem = pl.BlockSpec(memory_space=pltpu.VMEM)
    hbm = pl.BlockSpec(memory_space=pltpu.HBM)
    sems = [pltpu.SemaphoreType.DMA((k,)) for k in (3, S, S, T, T, S, S, T // 2, T // 2, T // 2, T // 2)]
    both = pl.pallas_call(
        functools.partial(body, rows, cols, side),
        out_shape=jax.ShapeDtypeStruct((2, n, max(wf, wc)), f32),
        in_specs=[hbm] * 3,
        out_specs=vmem,
        scratch_shapes=[
            pltpu.VMEM((S, height, wf), f32),
            pltpu.VMEM((T, height, wc), f32),
            pltpu.VMEM((4, n), f32),
            pltpu.VMEM((2, DEPTH, max(wf, wc)), f32),
            pltpu.VMEM((S, wf, DEPTH), bf16),
            pltpu.VMEM((T, DEPTH, wc), bf16),
            pltpu.VMEM((T, 2 * n, wc), bf16),
            pltpu.VMEM((S, 2 * n, wf), bf16),
            pltpu.VMEM((4, wf, wc), f32),
            pltpu.VMEM((4, wf, wc), bf16),
            pltpu.VMEM((4, wf, wc), bf16),
            pltpu.VMEM((S, n, wf), f32),
            pltpu.VMEM((S, n, wf), f32),
            pltpu.VMEM((T, n, wc), f32),
            pltpu.VMEM((T // 2, n, wc), f32),
            pltpu.VMEM((T // 2, n, wc), f32),
            *sems,
        ],
        compiler_params=pltpu.CompilerParams(
            collective_id=0, has_side_effects=True, vmem_limit_bytes=67_043_328
        ),
    )(fluid_data, center_data, poly_coef.T)
    return both[0, :, :wf], both[1, :, :wc]


def solution(mesh):
    rows, cols = mesh.shape["row"], mesh.shape["col"]
    side = 2 if cols % 2 == 0 else 1
    placed = (P(None, ("row", "col")), P(None, ("col", "row")), P())
    return jax.shard_map(
        functools.partial(per_device, rows, cols, side),
        mesh=mesh,
        in_specs=placed,
        out_specs=(P(None, ("row", "col")), P(None, ("col", "row"))),
        check_vma=False,
    )
```
